32 devices in a mesh: dp: 2 (over x), tp: 4 (over z), section: 4 (over y, core).
Axes of the slice: x: 2, y: 2, z: 4, core: 2. Of those that a mesh axis runs over, the one named last changes fastest.
Arguments:
- tokens: bfloat16 [256, 2304], P('dp', 'section'), may hold values from -6 to 6
- hidden_grad: bfloat16 [256, 18432], P('dp', ('tp', 'section')), may hold values from -6 to 6
- norm_gain: float32 [2304], replicated, may hold values from 0.5 to 1.5
- w_gate: bfloat16 [2304, 18432], P('dp', ('tp', 'section')), may hold values from -0.125 to 0.125
- w_up: bfloat16 [2304, 18432], P('dp', ('tp', 'section')), may hold values from -0.125 to 0.125
Outputs:
- grad_tokens: bfloat16 [256, 2304], P('dp', ('tp', 'section'))
- grad_gain: float32 [2304], P(('tp', 'section'))
- grad_gate: bfloat16 [2304, 18432], P('dp', ('tp', 'section'))
- grad_up: bfloat16 [2304, 18432], P('dp', ('tp', 'section'))
The draws below stay inside these ranges and needn't reach their ends.
All inputs are finite; a program needn't handle non-finite values.
Results may differ from the reference program's by a relative error of at most 0.018.
Values may be sent and summed in bfloat16 or wider, within the bound.
A program may use at most 128 MiB of HBM per device.

```python
import jax
import jax.numpy as jnp
from jax import lax

D = 2304
FF = 18432
TOK_DEV = 128
TOKENS = 256
N_DP = 2
N_TP = 4
N_SECTION = 4


def level_of(own_key, extent, cuts, smallest, top_value):
    gain, own = 1.0, jax.random.fold_in(own_key, 6)
    for position, shards_of in cuts:
        heights = jnp.exp(jax.random.uniform(jax.random.fold_in(own, position), (shards_of,), jnp.float32, smallest / len(cuts), top_value / len(cuts)))
        gain = gain * jnp.repeat(heights, extent[position] // shards_of).reshape([-1 if axis == position else 1 for axis in range(len(extent))])
    return gain


def centred(key, dims, deviation, bound, cuts=(), held_as=jnp.bfloat16):
    drawn = jax.random.normal(key, dims, jnp.float32) * deviation
    if len(cuts) > 0:
        drawn = level_of(key, dims, cuts, -0.22, 0.18) * drawn
    return jnp.clip(drawn, min=-bound, max=bound).astype(held_as)


def setup_inputs(seed: int = 0) -> dict:
    key_list = jax.random.split(jax.random.key(seed), 6)
    return {
        "tokens": centred(key_list[0], (TOKENS, D), 1.0, 6.0, ((0, 2), (1, 4))),
        "hidden_grad": centred(key_list[1], (TOKENS, FF), 1.0, 6.0, ((0, 2), (1, 16))),
        "norm_gain": jnp.clip(1.0 + 0.1 * jax.random.normal(key_list[2], (D,), jnp.float32), 0.5, 1.5),
        "w_gate": centred(key_list[3], (D, FF), D ** -0.5, 0.125, ((0, 2), (1, 16))),
        "w_up": centred(key_list[4], (D, FF), D ** -0.5, 0.125, ((0, 2), (1, 16))),
    }


epsilon = 1e-06

def gated_unit(gate, up):
    return jax.nn.gelu(gate, approximate=True) * up

def rounded(value):
    return lax.optimization_barrier(value.astype(jnp.bfloat16)).astype(jnp.float32)

def reference(tokens, hidden_grad, norm_gain, w_gate, w_up):
    groups = N_TP * N_SECTION
    fwidth = FF // groups
    gate_blocks = w_gate.astype(jnp.float32).reshape(D, groups, fwidth)
    up_blocks = w_up.astype(jnp.float32).reshape(D, groups, fwidth)

    def one_group(index, carry):
        sum_gate, sum_up, gain_total, result = carry
        start = (index * TOK_DEV).astype(jnp.int32)
        rows_in = lax.dynamic_slice_in_dim(tokens, start, TOK_DEV, 0)
        back = lax.dynamic_slice_in_dim(hidden_grad, start, TOK_DEV, 0).astype(jnp.float32)
        inputs = rows_in.astype(jnp.float32)
        inv_rms = lax.rsqrt(lax.optimization_barrier(jnp.mean(inputs * inputs, axis=1)) + epsilon)
        normed = (inputs * inv_rms[:, None] * norm_gain).astype(jnp.bfloat16)
        gate = jnp.dot(normed, w_gate, preferred_element_type=jnp.float32)
        up = jnp.dot(normed, w_up, preferred_element_type=jnp.float32)
        hidden, pull = jax.vjp(gated_unit, gate, up)
        d_gate, d_up = pull(back)
        d_gate = d_gate.astype(jnp.bfloat16)
        d_up = d_up.astype(jnp.bfloat16)
        gate_split = d_gate.astype(jnp.float32).reshape(TOK_DEV, groups, fwidth)
        up_split = d_up.astype(jnp.float32).reshape(TOK_DEV, groups, fwidth)
        parts = jnp.einsum('rbf,dbf->bdr', gate_split, gate_blocks) + jnp.einsum('rbf,dbf->bdr', up_split, up_blocks)
        d_normed = lax.optimization_barrier(jnp.sum(rounded(parts), axis=0)).T
        gain_total = gain_total + lax.optimization_barrier(jnp.sum(d_normed * inputs * inv_rms[:, None], axis=0))
        row_sum = lax.optimization_barrier(jnp.sum(inputs * norm_gain * d_normed, axis=1))
        grad_rows = inv_rms[:, None] * norm_gain * d_normed - inputs * (inv_rms ** 3 * row_sum / D)[:, None]
        result = lax.dynamic_update_slice(result, grad_rows.astype(jnp.bfloat16), (start, jnp.zeros((), jnp.int32)))
        sum_gate = sum_gate + rounded(jnp.dot(normed.T, d_gate, preferred_element_type=jnp.float32))
        sum_up = sum_up + rounded(jnp.dot(normed.T, d_up, preferred_element_type=jnp.float32))
        return (sum_gate, sum_up, gain_total, result)
    empty = jnp.zeros((D, FF), jnp.float32)
    start_carry = (empty, empty, jnp.zeros((D,), jnp.float32), jnp.zeros((TOKENS, D), jnp.bfloat16))
    sum_gate, sum_up, gain_total, result = lax.fori_loop(0, N_DP, one_group, start_carry)
    return (result, gain_total, sum_gate.astype(jnp.bfloat16), sum_up.astype(jnp.bfloat16))
```

```python
import functools

import jax
import jax.numpy as jnp
from jax import lax
from jax.experimental import pallas as pl
from jax.experimental.pallas import tpu as pltpu
from jax.sharding import PartitionSpec as P

D = 2304


epsilon = 1e-06


def gated_unit(gate, up):
    return jax.nn.gelu(gate, approximate=True) * up


def shards(tokens, hidden_grad, norm_gain, w_gate, w_up):
    n_dp = lax.axis_size("dp")
    n_model = lax.axis_size(("tp", "section"))
    rows_in = lax.all_gather(tokens, "section", axis=1, tiled=True)
    inputs = rows_in.astype(jnp.float32)
    inv_rms = lax.rsqrt(jnp.mean(inputs * inputs, axis=1) + epsilon)
    normed = (inputs * inv_rms[:, None] * norm_gain).astype(jnp.bfloat16)
    per_device, features = normed.shape
    cols_normed = lax.all_to_all(normed, "dp", split_axis=1, concat_axis=0, tiled=True)
    width = w_gate.shape[1]
    part_gate = jnp.dot(cols_normed, w_gate, preferred_element_type=jnp.float32)
    part_up = jnp.dot(cols_normed, w_up, preferred_element_type=jnp.float32)
    parts = jnp.concatenate([part_gate, part_up], axis=1).astype(jnp.bfloat16)
    parts = lax.all_to_all(parts, "dp", split_axis=0, concat_axis=0, tiled=True)
    sums = jnp.sum(parts.reshape(n_dp, per_device, 2 * width).astype(jnp.float32), axis=0)
    gate, up = sums[:, :width], sums[:, width:]
    hidden, pull = jax.vjp(gated_unit, gate, up)
    d_both = jnp.concatenate(pull(hidden_grad.astype(jnp.float32)), axis=1).astype(jnp.bfloat16)
    d_all = lax.all_gather(d_both, "dp", axis=0, tiled=True)
    d_gate, d_up = d_all[:, :width], d_all[:, width:]
    contract_cols = (((1,), (1,)), ((), ()))
    contract_rows = (((0,), (0,)), ((), ()))
    first = lax.dot_general(w_gate, d_gate, contract_cols, preferred_element_type=jnp.float32)
    second = lax.dot_general(w_up, d_up, contract_cols, preferred_element_type=jnp.float32)
    own_width = features // n_model
    per_row = n_model // n_dp
    d_part = (first + second).astype(jnp.bfloat16)
    d_part = d_part.reshape(per_row, own_width, n_dp, per_device).transpose(2, 0, 1, 3)
    d_part = d_part.reshape(n_model * own_width, per_device)
    d_columns = lax.psum_scatter(d_part, ("tp", "section"), scatter_dimension=0, tiled=True)
    moves = [
        (i * n_model + o * per_row + r, o * n_model + i * per_row + r)
        for i in range(n_dp)
        for o in range(n_dp)
        for r in range(per_row)
    ]
    d_columns = lax.ppermute(d_columns, ("dp", "tp", "section"), moves)
    d_normed = d_columns.astype(jnp.float32).T
    offset = lax.axis_index(("tp", "section")) * own_width
    own_inputs = lax.dynamic_slice_in_dim(inputs, offset, own_width, 1)
    own_gain = lax.dynamic_slice_in_dim(norm_gain, offset, own_width, 0)
    gain_part = jnp.sum(d_normed * own_inputs * inv_rms[:, None], axis=0)
    row_part = jnp.sum(own_inputs * own_gain * d_normed, axis=1)
    grad_gain = lax.psum(gain_part, "dp")
    row_sum = lax.psum(row_part, ("tp", "section"))
    grad_tokens = (
        inv_rms[:, None] * own_gain * d_normed
        - own_inputs * (inv_rms**3 * row_sum / features)[:, None]
    )
    grad_gate = lax.dot_general(cols_normed, d_gate, contract_rows, preferred_element_type=jnp.float32)
    grad_up = lax.dot_general(cols_normed, d_up, contract_rows, preferred_element_type=jnp.float32)
    return (
        grad_tokens.astype(jnp.bfloat16),
        grad_gain,
        grad_gate.astype(jnp.bfloat16),
        grad_up.astype(jnp.bfloat16),
    )


MESH = pl.DeviceIdType.MESH
SQRT_2_OVER_PI = 0.7978845608028654
CUBIC = 0.044715
CHUNKS = 3
HALVES = 2
CONTRACT_COLS = (((1,), (1,)), ((), ()))


def exchange_kernel(
    full,
    x_hbm,
    gain_hbm,
    back_hbm,
    wg_hbm,
    wu_hbm,
    grad_t,
    gain_out,
    grad_gate,
    grad_up,
    x_in,
    gain_in,
    gain_col,
    w,
    back,
    relay,
    xg,
    xs,
    xn,
    slab,
    squares,
    part_send,
    part_recv,
    own_part,
    d_all,
    own_pieces,
    own_sib,
    own_halved,
    own_incoming,
    pieces,
    sib_in,
    halved,
    incoming,
    move_send,
    moved,
    rows,
    prods,
    gains,
    load_sem,
    w_sem,
    tok_send,
    tok_recv,
    core_send,
    core_recv,
    slab_send,
    slab_recv,
    sq_send,
    sq_recv,
    part_ssem,
    part_rsem,
    d_ssem,
    d_rsem,
    own_ssem,
    own_rsem,
    piece_ssem,
    piece_rsem,
    sib_ssem,
    sib_rsem,
    last_send,
    last_recv,
    row_ssem,
    row_rsem,
):
    i, t, s = lax.axis_index("dp"), lax.axis_index("tp"), lax.axis_index("section")
    other = 1 - i
    f32, bf = jnp.float32, jnp.bfloat16
    sec_rows, per_device = x_in.shape
    own = slab.shape[0]
    block = 2 * sec_rows
    half, q = s // 2, lax.rem(s, 2)
    sibling, across = s + 1 - 2 * q, s + 2 - 4 * half
    ck = back.shape[2]
    th = per_device // HALVES
    fold = own // 2
    cut = sec_rows // 2
    reducer = t // 2 == i

    def to(d, tt, ss):
        return {"dp": d, "tp": tt, "section": ss}

    def send(src, dst, ssem, rsem, target):
        return pltpu.make_async_remote_copy(
            src_ref=src, dst_ref=dst, send_sem=ssem, recv_sem=rsem, device_id=target, device_id_type=MESH
        )

    barrier = pltpu.get_barrier_semaphore()
    group = [(dt, ds) for dt in range(4) for ds in range(4) if dt + ds > 0]
    everyone = [to(i, lax.rem(t + dt, 4), lax.rem(s + ds, 4)) for dt, ds in group]
    everyone += [to(other, t, s)]
    for target in everyone:
        pl.semaphore_signal(barrier, inc=1, device_id=target, device_id_type=MESH)

    x_load = pltpu.make_async_copy(x_hbm, x_in, load_sem.at[0])
    gain_load = pltpu.make_async_copy(gain_hbm, gain_in, load_sem.at[1])
    x_load.start()
    gain_load.start()
    loads = []
    for k in range(CHUNKS):
        cols = pl.ds(k * ck, ck)
        loads.append(
            (
                pltpu.make_async_copy(wg_hbm.at[:, cols], w.at[k, :, pl.ds(0, ck)], w_sem.at[0, k]),
                pltpu.make_async_copy(wu_hbm.at[:, cols], w.at[k, :, pl.ds(ck, ck)], w_sem.at[1, k]),
                pltpu.make_async_copy(back_hbm.at[:, cols], back.at[k], w_sem.at[2, k]),
            )
        )
        for load in loads[-1]:
            load.start()

    def seg(part):
        return pl.ds(pl.multiple_of(q * sec_rows + part * cut, 16), cut)

    my_rows = pl.ds(pl.multiple_of(q * sec_rows, 16), sec_rows)
    first, second = pl.ds(0, cut), pl.ds(cut, cut)
    xdev, ydev, cdev = to(other, t, s), to(i, t, across), to(i, t, sibling)

    def token_copy(n, m, src, dst, target):
        return send(src, dst, tok_send.at[n], tok_recv.at[m], target)

    x_first = token_copy(0, 0, x_in.at[first], xg.at[1, seg(0)], xdev)
    x_second = token_copy(1, 1, x_in.at[second], xg.at[1, seg(1)], xdev)
    y_second = token_copy(2, 3, x_in.at[second], relay, ydev)
    y_own = token_copy(0, 2, x_in, xg.at[0, my_rows], ydev)
    y_first = token_copy(1, 0, xg.at[1, seg(0)], xg.at[1, seg(0)], ydev)
    x_relay = token_copy(2, 1, relay, xg.at[1, seg(1)], xdev)
    core_own_in = send(x_in, xg.at[0, my_rows], core_send.at[2], core_recv.at[2], cdev)
    core_own = send(xg.at[0, my_rows], xg.at[0, my_rows], core_send.at[2], core_recv.at[2], cdev)
    core_other = [
        send(xg.at[1, seg(p)], xg.at[1, seg(p)], core_send.at[p], core_recv.at[p], cdev) for p in range(2)
    ]

    x_load.wait()
    raw = x_in[...].astype(f32)
    squares[0] = jnp.broadcast_to(jnp.sum(raw * raw, axis=0, keepdims=True), squares.shape[1:])

    pl.semaphore_wait(barrier, len(everyone))

    @pl.when(half != i)
    def _():
        x_first.start()
        y_second.start()
        x_second.start()

    @pl.when(half == i)
    def _():
        y_own.start()
        core_own_in.start()
        xg[0, my_rows] = x_in[...]

    square_sends = []
    for ds in range(1, 4):
        copy = send(
            squares.at[0], squares.at[ds], sq_send.at[ds], sq_recv.at[ds], to(i, t, lax.rem(s + ds, 4))
        )
        copy.start()
        square_sends.append(copy)

    def slab_copy(ds):
        ss = lax.rem(s + ds, 4)
        there = pl.ds(pl.multiple_of(ss * own, 16), own)
        return send(x_in.at[there], slab, slab_send.at[ds], slab_recv, to(i, t, ss))

    @pl.when(s == t)
    def _():
        for ds in range(1, 4):
            slab_copy(ds).start()
        slab[...] = x_in[pl.ds(pl.multiple_of(s * own, 16), own)]

    gain_load.wait()
    n_rows = gain_in.shape[0]
    filled = jnp.concatenate([gain_in[...], jnp.zeros((128 - n_rows, 128), f32)], axis=0).T
    for b in range(n_rows):
        gain_col[b * 128 : (b + 1) * 128] = jnp.broadcast_to(filled[:, b : b + 1], (128, 128))

    @pl.when(half == i)
    def _():
        x_first.wait_recv()
        y_first.start()

    @pl.when(half != i)
    def _():
        y_own.wait_recv()
        core_own.start()
        y_first.wait_recv()

    core_other[0].start()

    @pl.when(half == i)
    def _():
        y_second.wait_recv()
        x_relay.start()

    x_second.wait_recv()
    core_other[1].start()

    half_gain = gain_col.at[pl.ds(pl.multiple_of(i * block, 16), block)]

    def scale(slot):
        scaled = (xg[slot].astype(f32) * half_gain[...]).astype(bf)
        xs[:, slot * per_device : (slot + 1) * per_device] = scaled
        xn[slot] = scaled.T

    core_other[0].wait_recv()
    core_other[1].wait_recv()
    scale(1)
    part_sends = {}
    for h in range(HALVES):
        for k in range(CHUNKS):
            if h == 0:
                for load in loads[k]:
                    load.wait()
            part_send[h, k] = jnp.dot(
                xn[1, h * th : (h + 1) * th], w[k], preferred_element_type=f32
            ).astype(bf)
            copy = send(part_send.at[h, k], part_recv.at[h, k], part_ssem.at[h, k], part_rsem.at[h, k], xdev)
            copy.start()
            part_sends[h, k] = copy

    core_own.wait_recv()
    scale(0)
    for k in range(CHUNKS):
        own_part[k] = jnp.dot(xn[0], w[k], preferred_element_type=f32)
    for copy in square_sends:
        copy.wait()
    total = squares[0] + squares[1] + squares[2] + squares[3]
    inv_row = lax.rsqrt(total[:1] / full + epsilon)
    inv_all = jnp.broadcast_to(inv_row, (per_device, per_device)).T[:, :1]

    d_sends = {}
    row_cols = []
    for h in range(HALVES):
        here = slice(h * th, (h + 1) * th)
        inv = inv_all[here]
        row_col = jnp.zeros((th, 1), f32)
        for k in range(CHUNKS):
            part_sends[h, k].wait_recv()
            raw_sums = own_part[k, here] + part_recv[h, k].astype(f32)
            gate, up = raw_sums[:, :ck] * inv, raw_sums[:, ck:] * inv
            grad = back[k, here].astype(f32) * inv
            square = gate * gate
            tanh = jnp.tanh(SQRT_2_OVER_PI * gate * (1.0 + CUBIC * square))
            cdf = 0.5 * (1.0 + tanh)
            slope = cdf + 0.5 * gate * (1.0 - tanh * tanh) * (SQRT_2_OVER_PI * (1.0 + 3.0 * CUBIC * square))
            d_gate, d_up = grad * up * slope, grad * gate * cdf
            d_all[0, k, here, pl.ds(0, ck)] = d_gate.astype(bf)
            d_all[0, k, here, pl.ds(ck, ck)] = d_up.astype(bf)
            tokens_here = pl.ds(h * th, th)
            copy = send(
                d_all.at[0, k, tokens_here], d_all.at[1, k, tokens_here], d_ssem.at[h, k], d_rsem.at[h, k], xdev
            )
            copy.start()
            d_sends[h, k] = copy
            terms = d_gate * raw_sums[:, :ck] + d_up * raw_sums[:, ck:]
            row_col = row_col + jnp.sum(terms, axis=1, keepdims=True)
        row_cols.append(row_col)

    row_col = jnp.concatenate(row_cols, axis=0)
    rows[0] = jnp.broadcast_to(row_col, (per_device, per_device)).T[:8]
    row_sends = []
    for dt, ds in group:
        slot = dt * 4 + ds
        copy = send(
            rows.at[0],
            rows.at[slot],
            row_ssem.at[slot],
            row_rsem.at[slot],
            to(i, lax.rem(t + dt, 4), lax.rem(s + ds, 4)),
        )
        copy.start()
        row_sends.append(copy)

    def scatter(parts, landing, ssem, rsem):
        copies = []
        for e in (1, 0):
            tt = 2 * i + lax.rem(t + e, 2)
            dt = lax.rem(tt - t + 4, 4)
            for dy in (1, 0):
                ss = across if dy else s
                r = lax.rem(tt, 2) * 2 + ss // 2
                slot = dt * 2 + dy
                copy = send(parts.at[r], landing.at[slot], ssem.at[e * 2 + dy], rsem.at[slot], to(i, tt, ss))
                maybe_self = e == 0 and dy == 0
                if maybe_self:

                    @pl.when(dt == 0)
                    def _(r=r):
                        landing[0] = parts[r]

                    @pl.when(dt != 0)
                    def _(copy=copy):
                        copy.start()

                else:
                    copy.start()
                copies.append((copy, dt, maybe_self))
        return copies

    def gathered(parts, landing, ssem, rsem):
        for slot in range(1, 8):
            send(parts.at[0], landing.at[slot], ssem.at[0], rsem.at[slot], xdev).wait_recv()
        result = landing[0].astype(f32)
        for slot in range(1, 8):
            result = result + landing[slot].astype(f32)
        return result

    acc = None
    for k in range(CHUNKS):
        term = lax.dot_general(w[k], d_all[0, k], CONTRACT_COLS, preferred_element_type=f32)
        acc = term if acc is None else acc + term
    for r in range(8):
        own_pieces[r % 2, r // 2] = acc[r * own : (r + 1) * own].astype(bf)
    own_swap = send(own_pieces.at[1 - q], own_sib, sib_ssem.at[HALVES], sib_rsem.at[HALVES], cdev)
    own_swap.start()
    own_swap.wait_recv()
    own_halved[...] = (own_pieces[q].astype(f32) + own_sib[...].astype(f32)).astype(bf)
    piece_sends = scatter(own_halved, own_incoming, own_ssem, own_rsem)

    def weight_grads(k):
        both = jnp.concatenate([d_all[0, k], d_all[1, k]], axis=0)
        cols = pl.ds(k * ck, ck)
        grad_gate[:, cols] = jnp.dot(xs[...], both[:, :ck], preferred_element_type=f32).astype(bf)
        grad_up[:, cols] = jnp.dot(xs[...], both[:, ck:], preferred_element_type=f32).astype(bf)

    lane = lax.broadcasted_iota(jnp.int32, (fold, per_device), 1)
    left = lane < th
    swaps = []
    for h in range(HALVES):
        acc = None
        for k in range(CHUNKS):
            d_sends[h, k].wait_recv()
            late = d_all[1, k, h * th : (h + 1) * th]
            twice = jnp.concatenate([late, late], axis=0)
            term = lax.dot_general(w[k], twice, CONTRACT_COLS, preferred_element_type=f32)
            acc = term if acc is None else acc + term
            if h == HALVES - 1 and k < CHUNKS - 1:
                weight_grads(k)
        for r in range(8):
            upper, lower = acc[r * own : r * own + fold], acc[r * own + fold : (r + 1) * own]
            pieces[h, r % 2, r // 2] = jnp.where(left, upper, lower).astype(bf)
        swap = send(pieces.at[h, 1 - q], sib_in.at[h], sib_ssem.at[h], sib_rsem.at[h], cdev)
        swap.start()
        swap.wait_recv()
        swaps.append(swap)
        halved[h] = (pieces[h, q].astype(f32) + sib_in[h].astype(f32)).astype(bf)
        piece_sends += scatter(halved.at[h], incoming.at[h], piece_ssem.at[h], piece_rsem.at[h])

    weight_grads(CHUNKS - 1)
    for copy in row_sends:
        copy.wait()
    row_sum = rows[0]
    for slot in range(1, 16):
        row_sum = row_sum + rows[slot]
    factor = inv_row * inv_row * row_sum[:1] / full

    @pl.when(s != t)
    def _():
        slab_copy(1).wait_recv()

    mine = slab[...].astype(f32)
    gain_own = gain_col[pl.ds(pl.multiple_of((t * 4 + s) * own, 16), own)]

    def moves(h):
        return send(move_send.at[h], moved.at[h], last_send.at[h], last_recv.at[h], xdev)

    gain_copy = send(gains.at[0], gains.at[1], last_send.at[HALVES], last_recv.at[HALVES], xdev)

    @pl.when(reducer)
    def _():
        d_own = gathered(own_halved, own_incoming, own_ssem, own_rsem)
        grad_t[...] = (gain_own * d_own - mine * factor).astype(bf)
        prods[pl.ds(0, own)] = mine * d_own
        prods[pl.ds(own, prods.shape[0] - own)] = jnp.zeros((prods.shape[0] - own, per_device), f32)
        local = pl.multiple_of((lax.rem(t, 2) * 4 + s) * own, 16)
        theirs = xg[1, pl.ds(local, own)].astype(f32)
        upper, lower = theirs[:fold], theirs[fold:]
        for h in range(HALVES):
            d_late = gathered(halved.at[h], incoming.at[h], piece_ssem.at[h], piece_rsem.at[h])
            move_send[h] = d_late.astype(bf)
            moves(h).start()
            if h == 0:
                folded = jnp.where(left, upper, pltpu.roll(lower, th, 1))
            else:
                folded = jnp.where(left, pltpu.roll(upper, th, 1), lower)
            product = d_late * folded
            prods[pl.ds(0, fold)] += jnp.where(left, product, 0.0)
            prods[pl.ds(fold, fold)] += jnp.where(left, 0.0, product)
        gains[0] = jnp.broadcast_to(jnp.sum(prods[...].T, axis=0, keepdims=True), gains.shape[1:])
        gain_copy.start()
        gain_out[...] = gains[0, :1, :own]
        for h in range(HALVES):
            moves(h).wait_send()
        gain_copy.wait_send()

    @pl.when(jnp.logical_not(reducer))
    def _():
        moves(0).wait_recv()
        moves(1).wait_recv()
        early, late = moved[0].astype(f32), moved[1].astype(f32)
        upper = jnp.where(left, early, pltpu.roll(late, th, 1))
        lower = jnp.where(left, pltpu.roll(early, th, 1), late)
        grad_t[pl.ds(0, own)] = (
            gain_own * jnp.concatenate([upper, lower], axis=0) - mine * factor
        ).astype(bf)
        gain_copy.wait_recv()
        gain_out[...] = gains[1, :1, :own]

    @pl.when(half != i)
    def _():
        x_first.wait_send()
        y_second.wait_send()
        x_second.wait_send()
        core_own.wait_send()

    @pl.when(half == i)
    def _():
        y_own.wait_send()
        y_first.wait_send()
        x_relay.wait_send()
        core_own_in.wait_send()

    @pl.when(s == t)
    def _():
        for ds in range(1, 4):
            slab_copy(ds).wait_send()

    for copy in core_other + [own_swap] + swaps + list(part_sends.values()) + list(d_sends.values()):
        copy.wait_send()
    for copy, dt, maybe_self in piece_sends:
        if maybe_self:

            @pl.when(dt != 0)
            def _(copy=copy):
                copy.wait_send()

        else:
            copy.wait_send()


def write_kernel(grad_t, gain, grad_gate, grad_up, grad_t_out, gain_out, gate_out, up_out, sems):
    pairs = ((grad_gate, gate_out), (grad_up, up_out), (grad_t, grad_t_out), (gain, gain_out))
    copies = [pltpu.make_async_copy(src, dst, sems.at[n]) for n, (src, dst) in enumerate(pairs)]
    for copy in copies:
        copy.start()
    for copy in copies:
        copy.wait()


def fused_shards(tokens, hidden_grad, norm_gain, w_gate, w_up):
    per_device, sec_rows = tokens.shape
    block, width = w_gate.shape
    full = norm_gain.shape[0]
    own = full // 16
    ck = width // CHUNKS
    th = per_device // HALVES
    fold = own // 2
    bf, f32 = jnp.bfloat16, jnp.float32
    vmem = pl.BlockSpec(memory_space=pltpu.VMEM)
    anywhere = pl.BlockSpec(memory_space=pltpu.HBM)
    dma = pltpu.SemaphoreType.DMA
    own_pad = pl.cdiv(own, 128) * 128
    kept = (
        jax.ShapeDtypeStruct((own, per_device), bf),
        jax.ShapeDtypeStruct((1, own), f32),
        jax.ShapeDtypeStruct((block, width), bf),
        jax.ShapeDtypeStruct((block, width), bf),
    )
    operands = (tokens.T, norm_gain.reshape(full // 128, 128), hidden_grad, w_gate, w_up)
    results = pl.pallas_call(
        functools.partial(exchange_kernel, full),
        out_shape=tuple(pltpu.VMEM(a.shape, a.dtype) for a in kept),
        in_specs=[anywhere] * 5,
        out_specs=(vmem,) * 4,
        scratch_shapes=[
            pltpu.VMEM((sec_rows, per_device), bf),
            pltpu.VMEM((full // 128, 128), f32),
            pltpu.VMEM((full, 128), f32),
            pltpu.VMEM((CHUNKS, block, 2 * ck), bf),
            pltpu.VMEM((CHUNKS, per_device, ck), bf),
            pltpu.VMEM((sec_rows // 2, per_device), bf),
            pltpu.VMEM((2, block, per_device), bf),
            pltpu.VMEM((block, 2 * per_device), bf),
            pltpu.VMEM((2, per_device, block), bf),
            pltpu.VMEM((own, per_device), bf),
            pltpu.VMEM((4, 8, per_device), f32),
            pltpu.VMEM((HALVES, CHUNKS, th, 2 * ck), bf),
            pltpu.VMEM((HALVES, CHUNKS, th, 2 * ck), bf),
            pltpu.VMEM((CHUNKS, per_device, 2 * ck), f32),
            pltpu.VMEM((2, CHUNKS, per_device, 2 * ck), bf),
            pltpu.VMEM((2, 4, own, per_device), bf),
            pltpu.VMEM((4, own, per_device), bf),
            pltpu.VMEM((4, own, per_device), bf),
            pltpu.VMEM((8, own, per_device), bf),
            pltpu.VMEM((HALVES, 2, 4, fold, per_device), bf),
            pltpu.VMEM((HALVES, 4, fold, per_device), bf),
            pltpu.VMEM((HALVES, 4, fold, per_device), bf),
            pltpu.VMEM((HALVES, 8, fold, per_device), bf),
            pltpu.VMEM((HALVES, fold, per_device), bf),
            pltpu.VMEM((HALVES, fold, per_device), bf),
            pltpu.VMEM((16, 8, per_device), f32),
            pltpu.VMEM((own_pad, per_device), f32),
            pltpu.VMEM((2, 8, own_pad), f32),
            dma((2,)),
            dma((3, CHUNKS)),
            dma((3,)),
            dma((4,)),
            dma((3,)),
            dma((3,)),
            dma((4,)),
            dma,
            dma((4,)),
            dma((4,)),
            dma((HALVES, CHUNKS)),
            dma((HALVES, CHUNKS)),
            dma((HALVES, CHUNKS)),
            dma((HALVES, CHUNKS)),
            dma((4,)),
            dma((8,)),
            dma((HALVES, 4)),
            dma((HALVES, 8)),
            dma((HALVES + 1,)),
            dma((HALVES + 1,)),
            dma((HALVES + 1,)),
            dma((HALVES + 1,)),
            dma((16,)),
            dma((16,)),
        ],
        compiler_params=pltpu.CompilerParams(
            collective_id=0, has_side_effects=True, vmem_limit_bytes=KERNEL_MIB * 1024 * 1024
        ),
    )(*(pltpu.with_memory_space_constraint(a, pltpu.HBM) for a in operands))
    grad_t, gain, grad_gate, grad_up = pl.pallas_call(
        write_kernel,
        out_shape=kept,
        in_specs=[vmem] * 4,
        out_specs=(anywhere,) * 4,
        scratch_shapes=[dma((4,))],
        compiler_params=pltpu.CompilerParams(vmem_limit_bytes=16 * 1024 * 1024),
    )(*results)
    return grad_t.T, gain.reshape(own), grad_gate, grad_up


KERNEL_MIB = 40


def solution(mesh):
    in_specs = (
        P("dp", "section"),
        P("dp", ("tp", "section")),
        P(),
        P("dp", ("tp", "section")),
        P("dp", ("tp", "section")),
    )
    out_specs = (
        P("dp", ("tp", "section")),
        P(("tp", "section")),
        P("dp", ("tp", "section")),
        P("dp", ("tp", "section")),
    )
    sizes = tuple(mesh.shape[a] for a in ("dp", "tp", "section"))
    body = fused_shards if sizes == (2, 4, 4) else shards
    return jax.shard_map(body, mesh=mesh, in_specs=in_specs, out_specs=out_specs, check_vma=False)
```

```python
import functools

import jax
import jax.numpy as jnp
from jax import lax
from jax.experimental import pallas as pl
from jax.experimental.pallas import tpu as pltpu
from jax.sharding import PartitionSpec as P

D = 2304


epsilon = 1e-06


def gated_unit(gate, up):
    return jax.nn.gelu(gate, approximate=True) * up


def shards(tokens, hidden_grad, norm_gain, w_gate, w_up):
    n_dp = lax.axis_size("dp")
    n_model = lax.axis_size(("tp", "section"))
    rows_in = lax.all_gather(tokens, "section", axis=1, tiled=True)
    inputs = rows_in.astype(jnp.float32)
    inv_rms = lax.rsqrt(jnp.mean(inputs * inputs, axis=1) + epsilon)
    normed = (inputs * inv_rms[:, None] * norm_gain).astype(jnp.bfloat16)
    per_device, features = normed.shape
    cols_normed = lax.all_to_all(normed, "dp", split_axis=1, concat_axis=0, tiled=True)
    width = w_gate.shape[1]
    part_gate = jnp.dot(cols_normed, w_gate, preferred_element_type=jnp.float32)
    part_up = jnp.dot(cols_normed, w_up, preferred_element_type=jnp.float32)
    parts = jnp.concatenate([part_gate, part_up], axis=1).astype(jnp.bfloat16)
    parts = lax.all_to_all(parts, "dp", split_axis=0, concat_axis=0, tiled=True)
    sums = jnp.sum(parts.reshape(n_dp, per_device, 2 * width).astype(jnp.float32), axis=0)
    gate, up = sums[:, :width], sums[:, width:]
    hidden, pull = jax.vjp(gated_unit, gate, up)
    d_both = jnp.concatenate(pull(hidden_grad.astype(jnp.float32)), axis=1).astype(jnp.bfloat16)
    d_all = lax.all_gather(d_both, "dp", axis=0, tiled=True)
    d_gate, d_up = d_all[:, :width], d_all[:, width:]
    contract_cols = (((1,), (1,)), ((), ()))
    contract_rows = (((0,), (0,)), ((), ()))
    first = lax.dot_general(w_gate, d_gate, contract_cols, preferred_element_type=jnp.float32)
    second = lax.dot_general(w_up, d_up, contract_cols, preferred_element_type=jnp.float32)
    own_width = features // n_model
    per_row = n_model // n_dp
    d_part = (first + second).astype(jnp.bfloat16)
    d_part = d_part.reshape(per_row, own_width, n_dp, per_device).transpose(2, 0, 1, 3)
    d_part = d_part.reshape(n_model * own_width, per_device)
    d_columns = lax.psum_scatter(d_part, ("tp", "section"), scatter_dimension=0, tiled=True)
    moves = [
        (i * n_model + o * per_row + r, o * n_model + i * per_row + r)
        for i in range(n_dp)
        for o in range(n_dp)
        for r in range(per_row)
    ]
    d_columns = lax.ppermute(d_columns, ("dp", "tp", "section"), moves)
    d_normed = d_columns.astype(jnp.float32).T
    offset = lax.axis_index(("tp", "section")) * own_width
    own_inputs = lax.dynamic_slice_in_dim(inputs, offset, own_width, 1)
    own_gain = lax.dynamic_slice_in_dim(norm_gain, offset, own_width, 0)
    gain_part = jnp.sum(d_normed * own_inputs * inv_rms[:, None], axis=0)
    row_part = jnp.sum(own_inputs * own_gain * d_normed, axis=1)
    grad_gain = lax.psum(gain_part, "dp")
    row_sum = lax.psum(row_part, ("tp", "section"))
    grad_tokens = (
        inv_rms[:, None] * own_gain * d_normed
        - own_inputs * (inv_rms**3 * row_sum / features)[:, None]
    )
    grad_gate = lax.dot_general(cols_normed, d_gate, contract_rows, preferred_element_type=jnp.float32)
    grad_up = lax.dot_general(cols_normed, d_up, contract_rows, preferred_element_type=jnp.float32)
    return (
        grad_tokens.astype(jnp.bfloat16),
        grad_gain,
        grad_gate.astype(jnp.bfloat16),
        grad_up.astype(jnp.bfloat16),
    )


MESH = pl.DeviceIdType.MESH
SQRT_2_OVER_PI = 0.7978845608028654
CUBIC = 0.044715
CHUNKS = 3
HALVES = 2
CONTRACT_COLS = (((1,), (1,)), ((), ()))


def exchange_kernel(
    full,
    x_hbm,
    gain_hbm,
    back_hbm,
    wg_hbm,
    wu_hbm,
    grad_t,
    gain_out,
    grad_gate,
    grad_up,
    x_in,
    folded,
    gain_in,
    gain_col,
    w,
    back,
    relay,
    landed,
    xg,
    xs,
    xn,
    slab,
    squares,
    part_send,
    part_recv,
    own_part,
    d_all,
    own_pieces,
    own_sib,
    own_halved,
    own_incoming,
    pieces,
    sib_in,
    halved,
    incoming,
    move_send,
    moved,
    rows,
    prods,
    gains,
    far,
    load_sem,
    w_sem,
    tok_send,
    a_recv,
    b_recv,
    relay_recv,
    own_recv,
    core_send,
    core_recv,
    slab_sem,
    sq_sem,
    part_ssem,
    part_rsem,
    d_ssem,
    d_rsem,
    piece_ssem,
    piece_rsem,
    sib_ssem,
    sib_rsem,
    last_send,
    last_recv,
    row_sem,
):
    i, t, s = lax.axis_index("dp"), lax.axis_index("tp"), lax.axis_index("section")
    other = 1 - i
    f32, bf = jnp.float32, jnp.bfloat16
    sec_rows, per_device = x_in.shape
    own = slab.shape[0]
    block = 2 * sec_rows
    half, q = s // 2, lax.rem(s, 2)
    sibling, across = s + 1 - 2 * q, s + 2 - 4 * half
    ck = w.shape[2] // 2
    th = per_device // HALVES
    fold = own // 2
    flat = sec_rows // 2
    cut = flat // 2
    reducer = t // 2 == i
    not_reducer = jnp.logical_not(reducer)

    def to(d, tt, ss):
        return {"dp": d, "tp": tt, "section": ss}

    def send(src, dst, ssem, rsem, target):
        return pltpu.make_async_remote_copy(
            src_ref=src, dst_ref=dst, send_sem=ssem, recv_sem=rsem, device_id=target, device_id_type=MESH
        )

    xdev, ydev, cdev = to(other, t, s), to(i, t, across), to(i, t, sibling)

    def sent(ref, ssem):
        send(ref, ref, ssem, load_sem.at[0], xdev).wait_send()

    def received(ref, rsem):
        send(ref, ref, load_sem.at[0], rsem, xdev).wait_recv()

    barrier = pltpu.get_barrier_semaphore()
    near = [to(i, t, lax.rem(s + ds, 4)) for ds in range(1, 4)] + [xdev]
    z_near = 1 + (lax.rem(t, 3) + 2) // 3

    def signal_z(sem):
        @pl.when(t < 3)
        def _():
            pl.semaphore_signal(sem, inc=1, device_id=to(i, t + 1, s), device_id_type=MESH)

        @pl.when(t > 0)
        def _():
            pl.semaphore_signal(sem, inc=1, device_id=to(i, t - 1, s), device_id_type=MESH)

    x_load = pltpu.make_async_copy(x_hbm, x_in, load_sem.at[0])
    x_load.start()
    for target in near:
        pl.semaphore_signal(barrier, inc=1, device_id=target, device_id_type=MESH)
    signal_z(barrier)

    gain_load = pltpu.make_async_copy(gain_hbm, gain_in, load_sem.at[1])
    back_load = pltpu.make_async_copy(back_hbm, back, load_sem.at[2])
    loads = []
    for k in range(CHUNKS):
        cols = pl.ds(k * ck, ck)
        loads.append(
            (
                pltpu.make_async_copy(wg_hbm.at[:, cols], w.at[k, :, pl.ds(0, ck)], w_sem.at[0, k]),
                pltpu.make_async_copy(wu_hbm.at[:, cols], w.at[k, :, pl.ds(ck, ck)], w_sem.at[1, k]),
            )
        )

    def mine_at(n):
        return pl.ds(pl.multiple_of(q * flat + n * cut, 16), cut)

    my_rows = pl.ds(pl.multiple_of(q * sec_rows, 16), sec_rows)
    first, second = pl.ds(0, cut), pl.ds(cut, cut)
    x_first, x_second, y_second, y_first, x_relay, core_first, core_second, y_own = ([] for _ in range(8))
    for h in range(HALVES):
        a_here, b_here = landed.at[h, mine_at(0)], landed.at[h, mine_at(1)]
        x_first.append(send(folded.at[h, first], a_here, tok_send.at[0], a_recv.at[h], xdev))
        x_second.append(send(folded.at[h, second], b_here, tok_send.at[0], b_recv.at[h], xdev))
        y_second.append(send(folded.at[h, second], relay.at[h], tok_send.at[1], relay_recv.at[h], ydev))
        y_first.append(send(a_here, a_here, tok_send.at[1], a_recv.at[h], ydev))
        x_relay.append(send(relay.at[h], b_here, tok_send.at[2], b_recv.at[h], xdev))
        core_first.append(send(a_here, a_here, core_send.at[0], core_recv.at[h], cdev))
        core_second.append(send(b_here, b_here, core_send.at[0], core_recv.at[h], cdev))
        part = pl.ds(h * flat, flat)
        there = pl.ds(pl.multiple_of(q * sec_rows + h * flat, 16), flat)
        y_own.append(send(x_in.at[part], xg.at[0, there], tok_send.at[0], own_recv.at[h], ydev))
    core_own_in = send(x_in, xg.at[0, my_rows], core_send.at[1], core_recv.at[HALVES], cdev)
    core_own = send(xg.at[0, my_rows], xg.at[0, my_rows], core_send.at[1], core_recv.at[HALVES], cdev)
    left = lax.broadcasted_iota(jnp.int32, (flat, per_device), 1) < th
    left_own = lax.broadcasted_iota(jnp.int32, (fold, per_device), 1) < th

    x_load.wait()
    gain_load.start()
    for load in loads[0]:
        load.start()
    back_load.start()
    for k in range(1, CHUNKS):
        for load in loads[k]:
            load.start()
    raw = x_in[...].astype(f32)
    upper, lower = raw[:flat], raw[flat:]
    folded[0] = jnp.where(left, upper, pltpu.roll(lower, th, 1)).astype(bf)
    folded[1] = jnp.where(left, pltpu.roll(upper, th, 1), lower).astype(bf)
    squares[0] = jnp.broadcast_to(jnp.sum(raw * raw, axis=0, keepdims=True), squares.shape[1:])

    pl.semaphore_wait(barrier, len(near) + z_near)

    @pl.when(half != i)
    def _():
        for h in range(HALVES):
            x_first[h].start()
            y_second[h].start()
            x_second[h].start()

    @pl.when(half == i)
    def _():
        y_own[0].start()
        core_own_in.start()
        xg[0, my_rows] = x_in[...]

    signal_z(far.at[0])
    for ds in range(1, 4):
        send(squares.at[0], squares.at[ds], sq_sem.at[0], sq_sem.at[1], to(i, t, lax.rem(s + ds, 4))).start()

    gain_load.wait()
    n_rows = gain_in.shape[0]
    filled = jnp.concatenate([gain_in[...], jnp.zeros((128 - n_rows, 128), f32)], axis=0).T
    for b in range(n_rows):
        gain_col[b * 128 : (b + 1) * 128] = jnp.broadcast_to(filled[:, b : b + 1], (128, 128))

    @pl.when(half == i)
    def _():
        for h in range(HALVES):
            x_first[h].wait_recv()
            y_first[h].start()
            core_first[h].start()
            y_second[h].wait_recv()
            x_relay[h].start()
            if h == 0:
                y_own[1].start()
            x_second[h].wait_recv()
            core_second[h].start()

    @pl.when(half != i)
    def _():
        x_relay[0].wait_recv()
        core_second[0].start()
        y_first[0].wait_recv()
        core_first[0].start()

    half_gain = gain_col.at[pl.ds(pl.multiple_of(i * block, 16), block)]

    def unfold(h):
        sections = []
        for c in range(2):
            values = landed[h, c * flat : (c + 1) * flat].astype(f32)
            turned = pltpu.roll(values, th, 1)
            sections += [values, turned] if h == 0 else [turned, values]
        fresh = jnp.concatenate(sections, axis=0)
        if h > 0:
            wide = lax.broadcasted_iota(jnp.int32, fresh.shape, 1) < th
            fresh = jnp.where(wide, xg[1].astype(f32), fresh)
        xg[1] = fresh.astype(bf)
        scaled = (fresh * half_gain[...]).astype(bf)
        if h > 0:
            xs[:, per_device : 2 * per_device] = scaled
        xn[1, h * th : (h + 1) * th] = scaled.T[h * th : (h + 1) * th]

    part_sends, d_sends = {}, {}
    for h in range(HALVES):
        if h > 0:

            @pl.when(half != i)
            def _(h=h):
                x_relay[h].wait_recv()
                core_second[h].start()
                y_first[h].wait_recv()
                core_first[h].start()
                y_own[0].wait_recv()
                y_own[1].wait_recv()
                core_own.start()

        received(landed.at[h, pl.ds(0, flat)], core_recv.at[h])
        unfold(h)
        for k in range(CHUNKS):
            if h == 0:
                for load in loads[k]:
                    load.wait()
            part_send[h, k] = jnp.dot(
                xn[1, h * th : (h + 1) * th], w[k], preferred_element_type=f32
            ).astype(bf)
            copy = send(part_send.at[h, k], part_recv.at[h, k], part_ssem, part_rsem.at[h, k], xdev)
            copy.start()
            part_sends[h, k] = copy

    @pl.when(s == t)
    def _():
        for ds in range(1, 4):
            ss = lax.rem(s + ds, 4)
            there = pl.ds(pl.multiple_of(ss * own, 16), own)
            send(x_in.at[there], slab, slab_sem.at[0], slab_sem.at[1], to(i, t, ss)).start()
        slab[...] = x_in[pl.ds(pl.multiple_of(s * own, 16), own)]

    pl.semaphore_wait(far.at[0], z_near)
    signal_z(far.at[1])
    core_own.wait_recv()
    scaled = (xg[0].astype(f32) * half_gain[...]).astype(bf)
    xs[:, :per_device] = scaled
    xn[0] = scaled.T
    for k in range(CHUNKS):
        own_part[k] = jnp.dot(xn[0], w[k], preferred_element_type=f32)
    pl.semaphore_wait(far.at[1], z_near)
    signal_z(far.at[2])
    received(squares.at[pl.ds(1, 3)], sq_sem.at[1])
    total = squares[0] + squares[1] + squares[2] + squares[3]
    inv_row = lax.rsqrt(total[:1] / full + epsilon)
    inv_all = jnp.broadcast_to(inv_row, (per_device, per_device)).T[:, :1]
    back_load.wait()

    row_cols = []
    for h in range(HALVES):
        here = slice(h * th, (h + 1) * th)
        inv = inv_all[here]
        row_col = jnp.zeros((th, 1), f32)
        for k in range(CHUNKS):
            part_sends[h, k].wait_recv()
            raw_sums = own_part[k, here] + part_recv[h, k].astype(f32)
            gate, up = raw_sums[:, :ck] * inv, raw_sums[:, ck:] * inv
            grad = back[here, k * ck : (k + 1) * ck].astype(f32) * inv
            square = gate * gate
            tanh = jnp.tanh(SQRT_2_OVER_PI * gate * (1.0 + CUBIC * square))
            cdf = 0.5 * (1.0 + tanh)
            slope = cdf + 0.5 * gate * (1.0 - tanh * tanh) * (SQRT_2_OVER_PI * (1.0 + 3.0 * CUBIC * square))
            d_gate, d_up = grad * up * slope, grad * gate * cdf
            d_all[0, k, here, pl.ds(0, ck)] = d_gate.astype(bf)
            d_all[0, k, here, pl.ds(ck, ck)] = d_up.astype(bf)
            these = pl.ds(h * th, th)
            copy = send(d_all.at[0, k, these], d_all.at[1, k, these], d_ssem, d_rsem.at[h, k], xdev)
            copy.start()
            d_sends[h, k] = copy
            terms = d_gate * raw_sums[:, :ck] + d_up * raw_sums[:, ck:]
            row_col = row_col + jnp.sum(terms, axis=1, keepdims=True)
        row_cols.append(row_col)

    row_col = jnp.concatenate(row_cols, axis=0)
    rows[0] = jnp.broadcast_to(row_col, (per_device, per_device)).T[:8]
    pl.semaphore_wait(far.at[2], z_near)
    for dt in range(4):
        for ds in range(4):
            if dt + ds > 0:
                target = to(i, lax.rem(t + dt, 4), lax.rem(s + ds, 4))
                send(rows.at[0], rows.at[dt * 4 + ds], row_sem.at[0], row_sem.at[1], target).start()

    def scatter(parts, landing, n):
        for e in (1, 0):
            tt = 2 * i + lax.rem(t + e, 2)
            dt = lax.rem(tt - t + 4, 4)
            for dy in (1, 0):
                ss = across if dy else s
                r = lax.rem(tt, 2) * 2 + ss // 2
                slot = dt * 2 + dy
                copy = send(parts.at[r], landing.at[slot], piece_ssem.at[n], piece_rsem.at[n], to(i, tt, ss))
                if e == 0 and dy == 0:

                    @pl.when(reducer)
                    def _(r=r):
                        landing[0] = parts[r]

                    @pl.when(not_reducer)
                    def _(copy=copy):
                        copy.start()

                else:
                    copy.start()

    def scattered(parts, n):
        @pl.when(reducer)
        def _():
            sent(parts.at[pl.ds(0, 3)], piece_ssem.at[n])

        @pl.when(not_reducer)
        def _():
            sent(parts, piece_ssem.at[n])

    def gathered(landing, n):
        received(landing.at[pl.ds(1, 7)], piece_rsem.at[n])
        result = landing[0].astype(f32)
        for slot in range(1, 8):
            result = result + landing[slot].astype(f32)
        return result

    acc = None
    for k in range(CHUNKS):
        term = lax.dot_general(w[k], d_all[0, k], CONTRACT_COLS, preferred_element_type=f32)
        acc = term if acc is None else acc + term
    for r in range(8):
        own_pieces[r % 2, r // 2] = acc[r * own : (r + 1) * own].astype(bf)
    own_swap = send(own_pieces.at[1 - q], own_sib, sib_ssem.at[HALVES], sib_rsem.at[HALVES], cdev)
    own_swap.start()
    own_swap.wait_recv()
    own_halved[...] = (own_pieces[q].astype(f32) + own_sib[...].astype(f32)).astype(bf)
    scatter(own_halved, own_incoming, HALVES)

    def weight_grads(k):
        both = jnp.concatenate([d_all[0, k], d_all[1, k]], axis=0)
        cols = pl.ds(k * ck, ck)
        grads = jnp.dot(xs[...], both, preferred_element_type=f32).astype(bf)
        grad_gate[:, cols] = grads[:, :ck]
        grad_up[:, cols] = grads[:, ck:]

    swaps = []
    for h in range(HALVES):
        acc = None
        for k in range(CHUNKS):
            d_sends[h, k].wait_recv()
            late = d_all[1, k, h * th : (h + 1) * th]
            twice = jnp.concatenate([late, late], axis=0)
            term = lax.dot_general(w[k], twice, CONTRACT_COLS, preferred_element_type=f32)
            acc = term if acc is None else acc + term
            if h == HALVES - 1 and k == 0:
                weight_grads(0)
        for r in range(8):
            top, bottom = acc[r * own : r * own + fold], acc[r * own + fold : (r + 1) * own]
            pieces[h, r % 2, r // 2] = jnp.where(left_own, top, bottom).astype(bf)
        swap = send(pieces.at[h, 1 - q], sib_in.at[h], sib_ssem.at[h], sib_rsem.at[h], cdev)
        swap.start()
        if h == HALVES - 1:
            weight_grads(1)
        swap.wait_recv()
        swaps.append(swap)
        halved[h] = (pieces[h, q].astype(f32) + sib_in[h].astype(f32)).astype(bf)
        scatter(halved.at[h], incoming.at[h], h)

    weight_grads(CHUNKS - 1)
    received(rows.at[pl.ds(1, 15)], row_sem.at[1])
    row_sum = rows[0]
    for slot in range(1, 16):
        row_sum = row_sum + rows[slot]
    factor = inv_row * inv_row * row_sum[:1] / full

    @pl.when(s != t)
    def _():
        received(slab, slab_sem.at[1])

    mine = slab[...].astype(f32)
    gain_own = gain_col[pl.ds(pl.multiple_of((t * 4 + s) * own, 16), own)]

    def moves(h):
        return send(move_send.at[h], moved.at[h], last_send.at[0], last_recv.at[h], xdev)

    gain_copy = send(gains.at[0], gains.at[1], last_send.at[1], last_recv.at[HALVES], xdev)

    @pl.when(reducer)
    def _():
        d_own = gathered(own_incoming, HALVES)
        grad_t[...] = (gain_own * d_own - mine * factor).astype(bf)
        prods[pl.ds(0, own)] = mine * d_own
        prods[pl.ds(own, prods.shape[0] - own)] = jnp.zeros((prods.shape[0] - own, per_device), f32)
        local = pl.multiple_of((lax.rem(t, 2) * 4 + s) * own, 16)
        theirs = xg[1, pl.ds(local, own)].astype(f32)
        top, bottom = theirs[:fold], theirs[fold:]
        for h in range(HALVES):
            d_late = gathered(incoming.at[h], h)
            move_send[h] = d_late.astype(bf)
            moves(h).start()
            if h == 0:
                match = jnp.where(left_own, top, pltpu.roll(bottom, th, 1))
            else:
                match = jnp.where(left_own, pltpu.roll(top, th, 1), bottom)
            product = d_late * match
            prods[pl.ds(0, fold)] += jnp.where(left_own, product, 0.0)
            prods[pl.ds(fold, fold)] += jnp.where(left_own, 0.0, product)
        gains[0] = jnp.broadcast_to(jnp.sum(prods[...].T, axis=0, keepdims=True), gains.shape[1:])
        gain_copy.start()
        gain_out[...] = gains[0, :1, :own]

    def drain():
        @pl.when(half != i)
        def _():
            sent(folded, tok_send.at[0])
            sent(relay, tok_send.at[1])

        @pl.when(half == i)
        def _():
            sent(x_in, tok_send.at[0])
            sent(relay, tok_send.at[1])
            sent(relay, tok_send.at[2])

        sent(folded, core_send.at[0])
        sent(x_in, core_send.at[1])

        @pl.when(s == t)
        def _():
            sent(x_in.at[pl.ds(0, 3 * own)], slab_sem.at[0])

        sent(squares.at[pl.ds(1, 3)], sq_sem.at[0])
        sent(part_send, part_ssem)
        sent(d_all.at[0], d_ssem)
        sent(rows.at[pl.ds(1, 15)], row_sem.at[0])
        for copy in [own_swap] + swaps:
            copy.wait_send()
        scattered(own_halved, HALVES)
        for h in range(HALVES):
            scattered(halved.at[h], h)

    drain()

    @pl.when(reducer)
    def _():
        sent(move_send, last_send.at[0])
        gain_copy.wait_send()

    @pl.when(not_reducer)
    def _():
        moves(0).wait_recv()
        moves(1).wait_recv()
        early, final = moved[0].astype(f32), moved[1].astype(f32)
        top = jnp.where(left_own, early, pltpu.roll(final, th, 1))
        bottom = jnp.where(left_own, pltpu.roll(early, th, 1), final)
        grad_t[...] = (gain_own * jnp.concatenate([top, bottom], axis=0) - mine * factor).astype(bf)
        gain_copy.wait_recv()
        gain_out[...] = gains[1, :1, :own]


WRITES = 4


def write_kernel(grad_t, gain, grad_gate, grad_up, grad_t_out, gain_out, gate_out, up_out, sems):
    pairs = [(grad_t, grad_t_out), (gain, gain_out)]
    n = grad_gate.shape[0] // WRITES
    for p in range(WRITES):
        part = pl.ds(p * n, n)
        pairs += [(grad_gate.at[part], gate_out.at[part]), (grad_up.at[part], up_out.at[part])]
    copies = [pltpu.make_async_copy(src, dst, sems.at[n]) for n, (src, dst) in enumerate(pairs)]
    for copy in copies:
        copy.start()
    for copy in copies:
        copy.wait()


def fused_shards(tokens, hidden_grad, norm_gain, w_gate, w_up):
    per_device, sec_rows = tokens.shape
    block, width = w_gate.shape
    full = norm_gain.shape[0]
    own = full // 16
    ck = width // CHUNKS
    th = per_device // HALVES
    fold = own // 2
    flat = sec_rows // 2
    bf, f32 = jnp.bfloat16, jnp.float32
    vmem = pl.BlockSpec(memory_space=pltpu.VMEM)
    anywhere = pl.BlockSpec(memory_space=pltpu.HBM)
    dma = pltpu.SemaphoreType.DMA
    own_pad = pl.cdiv(own, 128) * 128
    kept = (
        jax.ShapeDtypeStruct((own, per_device), bf),
        jax.ShapeDtypeStruct((1, own), f32),
        jax.ShapeDtypeStruct((block, width), bf),
        jax.ShapeDtypeStruct((block, width), bf),
    )
    operands = (tokens.T, norm_gain.reshape(full // 128, 128), hidden_grad, w_gate, w_up)
    results = pl.pallas_call(
        functools.partial(exchange_kernel, full),
        out_shape=tuple(pltpu.VMEM(a.shape, a.dtype) for a in kept),
        in_specs=[anywhere] * 5,
        out_specs=(vmem,) * 4,
        scratch_shapes=[
            pltpu.VMEM((sec_rows, per_device), bf),
            pltpu.VMEM((HALVES, flat, per_device), bf),
            pltpu.VMEM((full // 128, 128), f32),
            pltpu.VMEM((full, 128), f32),
            pltpu.VMEM((CHUNKS, block, 2 * ck), bf),
            pltpu.VMEM((per_device, width), bf),
            pltpu.VMEM((HALVES, flat // 2, per_device), bf),
            pltpu.VMEM((HALVES, 2 * flat, per_device), bf),
            pltpu.VMEM((2, block, per_device), bf),
            pltpu.VMEM((block, 2 * per_device), bf),
            pltpu.VMEM((2, per_device, block), bf),
            pltpu.VMEM((own, per_device), bf),
            pltpu.VMEM((4, 8, per_device), f32),
            pltpu.VMEM((HALVES, CHUNKS, th, 2 * ck), bf),
            pltpu.VMEM((HALVES, CHUNKS, th, 2 * ck), bf),
            pltpu.VMEM((CHUNKS, per_device, 2 * ck), f32),
            pltpu.VMEM((2, CHUNKS, per_device, 2 * ck), bf),
            pltpu.VMEM((2, 4, own, per_device), bf),
            pltpu.VMEM((4, own, per_device), bf),
            pltpu.VMEM((4, own, per_device), bf),
            pltpu.VMEM((8, own, per_device), bf),
            pltpu.VMEM((HALVES, 2, 4, fold, per_device), bf),
            pltpu.VMEM((HALVES, 4, fold, per_device), bf),
            pltpu.VMEM((HALVES, 4, fold, per_device), bf),
            pltpu.VMEM((HALVES, 8, fold, per_device), bf),
            pltpu.VMEM((HALVES, fold, per_device), bf),
            pltpu.VMEM((HALVES, fold, per_device), bf),
            pltpu.VMEM((16, 8, per_device), f32),
            pltpu.VMEM((own_pad, per_device), f32),
            pltpu.VMEM((2, 8, own_pad), f32),
            pltpu.SemaphoreType.REGULAR((3,)),
            dma((3,)),
            dma((2, CHUNKS)),
            dma((3,)),
            dma((HALVES,)),
            dma((HALVES,)),
            dma((HALVES,)),
            dma((HALVES,)),
            dma((2,)),
            dma((HALVES + 1,)),
            dma((2,)),
            dma((2,)),
            dma,
            dma((HALVES, CHUNKS)),
            dma,
            dma((HALVES, CHUNKS)),
            dma((HALVES + 1,)),
            dma((HALVES + 1,)),
            dma((HALVES + 1,)),
            dma((HALVES + 1,)),
            dma((2,)),
            dma((HALVES + 1,)),
            dma((2,)),
        ],
        compiler_params=pltpu.CompilerParams(
            collective_id=0, has_side_effects=True, vmem_limit_bytes=40 * 1024 * 1024
        ),
    )(*(pltpu.with_memory_space_constraint(a, pltpu.HBM) for a in operands))
    grad_t, gain, grad_gate, grad_up = pl.pallas_call(
        write_kernel,
        out_shape=kept,
        in_specs=[vmem] * 4,
        out_specs=(anywhere,) * 4,
        scratch_shapes=[dma((2 * WRITES + 2,))],
        compiler_params=pltpu.CompilerParams(vmem_limit_bytes=16 * 1024 * 1024),
    )(*results)
    return grad_t.T, gain.reshape(own), grad_gate, grad_up


def solution(mesh):
    in_specs = (
        P("dp", "section"),
        P("dp", ("tp", "section")),
        P(),
        P("dp", ("tp", "section")),
        P("dp", ("tp", "section")),
    )
    out_specs = (
        P("dp", ("tp", "section")),
        P(("tp", "section")),
        P("dp", ("tp", "section")),
        P("dp", ("tp", "section")),
    )
    sizes = tuple(mesh.shape[a] for a in ("dp", "tp", "section"))
    body = fused_shards if sizes == (2, 4, 4) else shards
    return jax.shard_map(body, mesh=mesh, in_specs=in_specs, out_specs=out_specs, check_vma=False)
```

```python
import functools

import jax
import jax.numpy as jnp
from jax import lax
from jax.experimental import pallas as pl
from jax.experimental.pallas import tpu as pltpu
from jax.sharding import PartitionSpec as P

D = 2304


epsilon = 1e-06


def gated_unit(gate, up):
    return jax.nn.gelu(gate, approximate=True) * up


def shards(tokens, hidden_grad, norm_gain, w_gate, w_up):
    n_dp = lax.axis_size("dp")
    n_model = lax.axis_size(("tp", "section"))
    rows_in = lax.all_gather(tokens, "section", axis=1, tiled=True)
    inputs = rows_in.astype(jnp.float32)
    inv_rms = lax.rsqrt(jnp.mean(inputs * inputs, axis=1) + epsilon)
    normed = (inputs * inv_rms[:, None] * norm_gain).astype(jnp.bfloat16)
    per_device, features = normed.shape
    cols_normed = lax.all_to_all(normed, "dp", split_axis=1, concat_axis=0, tiled=True)
    width = w_gate.shape[1]
    part_gate = jnp.dot(cols_normed, w_gate, preferred_element_type=jnp.float32)
    part_up = jnp.dot(cols_normed, w_up, preferred_element_type=jnp.float32)
    parts = jnp.concatenate([part_gate, part_up], axis=1).astype(jnp.bfloat16)
    parts = lax.all_to_all(parts, "dp", split_axis=0, concat_axis=0, tiled=True)
    sums = jnp.sum(parts.reshape(n_dp, per_device, 2 * width).astype(jnp.float32), axis=0)
    gate, up = sums[:, :width], sums[:, width:]
    hidden, pull = jax.vjp(gated_unit, gate, up)
    d_both = jnp.concatenate(pull(hidden_grad.astype(jnp.float32)), axis=1).astype(jnp.bfloat16)
    d_all = lax.all_gather(d_both, "dp", axis=0, tiled=True)
    d_gate, d_up = d_all[:, :width], d_all[:, width:]
    contract_cols = (((1,), (1,)), ((), ()))
    contract_rows = (((0,), (0,)), ((), ()))
    first = lax.dot_general(w_gate, d_gate, contract_cols, preferred_element_type=jnp.float32)
    second = lax.dot_general(w_up, d_up, contract_cols, preferred_element_type=jnp.float32)
    own_width = features // n_model
    per_row = n_model // n_dp
    d_part = (first + second).astype(jnp.bfloat16)
    d_part = d_part.reshape(per_row, own_width, n_dp, per_device).transpose(2, 0, 1, 3)
    d_part = d_part.reshape(n_model * own_width, per_device)
    d_columns = lax.psum_scatter(d_part, ("tp", "section"), scatter_dimension=0, tiled=True)
    moves = [
        (i * n_model + o * per_row + r, o * n_model + i * per_row + r)
        for i in range(n_dp)
        for o in range(n_dp)
        for r in range(per_row)
    ]
    d_columns = lax.ppermute(d_columns, ("dp", "tp", "section"), moves)
    d_normed = d_columns.astype(jnp.float32).T
    offset = lax.axis_index(("tp", "section")) * own_width
    own_inputs = lax.dynamic_slice_in_dim(inputs, offset, own_width, 1)
    own_gain = lax.dynamic_slice_in_dim(norm_gain, offset, own_width, 0)
    gain_part = jnp.sum(d_normed * own_inputs * inv_rms[:, None], axis=0)
    row_part = jnp.sum(own_inputs * own_gain * d_normed, axis=1)
    grad_gain = lax.psum(gain_part, "dp")
    row_sum = lax.psum(row_part, ("tp", "section"))
    grad_tokens = (
        inv_rms[:, None] * own_gain * d_normed
        - own_inputs * (inv_rms**3 * row_sum / features)[:, None]
    )
    grad_gate = lax.dot_general(cols_normed, d_gate, contract_rows, preferred_element_type=jnp.float32)
    grad_up = lax.dot_general(cols_normed, d_up, contract_rows, preferred_element_type=jnp.float32)
    return (
        grad_tokens.astype(jnp.bfloat16),
        grad_gain,
        grad_gate.astype(jnp.bfloat16),
        grad_up.astype(jnp.bfloat16),
    )


MESH = pl.DeviceIdType.MESH
SQRT_2_OVER_PI = 0.7978845608028654
CUBIC = 0.044715
CHUNKS = 3
SENT_GROUPS = ((0, 32), (32, 32), (64, 64))
LATE_GROUPS = ((0, 64), (64, 32), (96, 32))


def spans(own, ways):
    tall = pl.cdiv(own // ways, 8) * 8
    count = (own - ways * (tall - 8)) // 8
    lengths = [tall if j < count else tall - 8 for j in range(ways)]
    return [(sum(lengths[:j]), lengths[j]) for j in range(ways)]


def exchange_kernel(
    full,
    x_hbm,
    gain_hbm,
    back_hbm,
    wg_hbm,
    wu_hbm,
    grad_t,
    gain_out,
    grad_gate,
    grad_up,
    x_in,
    folded,
    landed,
    gain_in,
    gain_col,
    w,
    w_t,
    back,
    xg,
    xs,
    xn,
    slab,
    squares,
    part_send,
    part_recv,
    own_part,
    d_all,
    own_pieces,
    own_sib,
    own_halved,
    own_incoming,
    late_bufs,
    rows,
    prods,
    gains,
    far,
    load_sem,
    w_sem,
    tok_send,
    tok_recv,
    core_send,
    core_recv,
    slab_sem,
    sq_sem,
    part_ssem,
    part_rsem,
    d_ssem,
    d_rsem,
    piece_ssem,
    piece_rsem,
    sib_ssem,
    sib_rsem,
    last_send,
    last_recv,
    row_sem,
):
    i, t, s = lax.axis_index("dp"), lax.axis_index("tp"), lax.axis_index("section")
    other = 1 - i
    f32, bf = jnp.float32, jnp.bfloat16
    sec_rows, per_device = x_in.shape
    own = slab.shape[0]
    block = 2 * sec_rows
    half, q = s // 2, lax.rem(s, 2)
    sibling, across = s + 1 - 2 * q, s + 2 - 4 * half
    ck = w.shape[2] // 2
    n_sent, n_late = len(SENT_GROUPS), len(LATE_GROUPS)
    lane = lax.broadcasted_iota(jnp.int32, (1, per_device), 1)
    reducer = t // 2 == i
    not_reducer = jnp.logical_not(reducer)

    def to(d, tt, ss):
        return {"dp": d, "tp": tt, "section": ss}

    def send(src, dst, ssem, rsem, target):
        return pltpu.make_async_remote_copy(
            src_ref=src, dst_ref=dst, send_sem=ssem, recv_sem=rsem, device_id=target, device_id_type=MESH
        )

    xdev, ydev, cdev = to(other, t, s), to(i, t, across), to(i, t, sibling)
    diagonal = to(other, t, across)

    def turn(value, shift):
        shift = shift % per_device
        return pltpu.roll(value, shift, 1) if shift else value

    def pick(parts, size):
        result = parts[0]
        for j in range(1, len(parts)):
            result = jnp.where(lane >= j * size, parts[j], result)
        return result

    def sent(ref, ssem):
        send(ref, ref, ssem, load_sem.at[0], xdev).wait_send()

    def received(ref, rsem):
        send(ref, ref, load_sem.at[0], rsem, xdev).wait_recv()

    barrier = pltpu.get_barrier_semaphore()
    near = [to(i, t, lax.rem(s + ds, 4)) for ds in range(1, 4)] + [xdev, diagonal]
    z_near = 1 + (lax.rem(t, 3) + 2) // 3

    def signal_z(sem):
        @pl.when(t < 3)
        def _():
            pl.semaphore_signal(sem, inc=1, device_id=to(i, t + 1, s), device_id_type=MESH)

        @pl.when(t > 0)
        def _():
            pl.semaphore_signal(sem, inc=1, device_id=to(i, t - 1, s), device_id_type=MESH)

    x_load = pltpu.make_async_copy(x_hbm, x_in, load_sem.at[0])
    x_load.start()
    gain_load = pltpu.make_async_copy(gain_hbm, gain_in, load_sem.at[1])
    gain_load.start()
    for target in near:
        pl.semaphore_signal(barrier, inc=1, device_id=target, device_id_type=MESH)
    signal_z(barrier)

    back_load = pltpu.make_async_copy(back_hbm, back, load_sem.at[2])
    loads = []
    for k in range(CHUNKS):
        cols = pl.ds(k * ck, ck)
        loads.append(
            (
                pltpu.make_async_copy(wg_hbm.at[:, cols], w.at[k, :, pl.ds(0, ck)], w_sem.at[0, k]),
                pltpu.make_async_copy(wu_hbm.at[:, cols], w.at[k, :, pl.ds(ck, ck)], w_sem.at[1, k]),
            )
        )

    my_rows = pl.ds(pl.multiple_of(q * sec_rows, 16), sec_rows)
    to_near, to_far, to_core = [], [], []
    for g in range(n_sent):
        n = folded[g].shape[0]
        here = landed[g].at[pl.ds(pl.multiple_of(q * n, 16), n)]
        to_near.append(send(folded[g], here, tok_send.at[0], tok_recv.at[g], xdev))
        to_far.append(send(folded[g], here, tok_send.at[1], tok_recv.at[g], diagonal))
        to_core.append(send(here, here, core_send.at[0], core_recv.at[g], cdev))
    y_own = send(x_in, xg.at[0, my_rows], tok_send.at[0], tok_recv.at[n_sent], ydev)
    core_own_in = send(x_in, xg.at[0, my_rows], core_send.at[1], core_recv.at[n_sent], cdev)
    core_own = send(xg.at[0, my_rows], xg.at[0, my_rows], core_send.at[1], core_recv.at[n_sent], cdev)

    x_load.wait()
    for load in loads[0]:
        load.start()
    back_load.start()
    for k in range(1, CHUNKS):
        for load in loads[k]:
            load.start()
    raw = x_in[...].astype(f32)
    for g, (start, size) in enumerate(SENT_GROUPS):
        n = folded[g].shape[0]
        ways = per_device // size
        parts = [turn(raw[j * n : (j + 1) * n], j * size - start) for j in range(ways)]
        folded[g][...] = pick(parts, size).astype(bf)
    squares[0] = jnp.broadcast_to(jnp.sum(raw * raw, axis=0, keepdims=True), squares.shape[1:])

    pl.semaphore_wait(barrier, len(near) + z_near)

    @pl.when(half != i)
    def _():
        for g in range(n_sent):
            to_far[g].start()
            to_near[g].start()

    @pl.when(half == i)
    def _():
        core_own_in.start()
        xg[0, my_rows] = x_in[...]

    signal_z(far.at[0])
    for ds in range(1, 4):
        send(squares.at[0], squares.at[ds], sq_sem.at[0], sq_sem.at[1], to(i, t, lax.rem(s + ds, 4))).start()

    gain_load.wait()
    n_rows = gain_in.shape[0]
    filled = jnp.concatenate([gain_in[...], jnp.zeros((128 - n_rows, 128), f32)], axis=0).T
    for b in range(n_rows):
        gain_col[b * 128 : (b + 1) * 128] = jnp.broadcast_to(filled[:, b : b + 1], (128, 128))

    for k in range(CHUNKS):
        for load in loads[k]:
            load.wait()
        w_t[k] = w[k].T

    half_gain = gain_col.at[pl.ds(pl.multiple_of(i * block, 16), block)]

    def unfold(g):
        start, size = SENT_GROUPS[g]
        n = folded[g].shape[0]
        parts = []
        for c in range(2):
            values = landed[g][c * n : (c + 1) * n].astype(f32)
            parts += [turn(values, start - j * size) for j in range(per_device // size)]
        fresh = jnp.concatenate(parts, axis=0)
        if g > 0:
            fresh = jnp.where(lane >= start, fresh, xg[1].astype(f32))
        xg[1] = fresh.astype(bf)
        scaled = (fresh * half_gain[...]).astype(bf)
        if g == n_sent - 1:
            xs[:, per_device : 2 * per_device] = scaled
        xn[1, start : start + size] = scaled.T[start : start + size]

    def forward(g):
        to_near[g].wait_recv()
        to_core[g].start()

    part_sends, d_sends = {}, {}
    forward(0)

    @pl.when(half == i)
    def _():
        y_own.start()

    for g, (start, size) in enumerate(SENT_GROUPS):
        to_core[g].wait_recv()
        unfold(g)
        these = pl.ds(start, size)
        for k in range(CHUNKS):
            part_send[k, these] = jnp.dot(
                xn[1, start : start + size], w[k], preferred_element_type=f32
            ).astype(bf)
            copy = send(part_send.at[k, these], part_recv.at[k, these], part_ssem, part_rsem.at[g, k], xdev)
            copy.start()
            part_sends[g, k] = copy
            if k == 0 and g < n_sent - 1:
                forward(g + 1)
            if k == 1 and g == n_sent - 1:

                @pl.when(half != i)
                def _():
                    y_own.wait_recv()
                    core_own.start()

    @pl.when(s == t)
    def _():
        for ds in range(1, 4):
            ss = lax.rem(s + ds, 4)
            there = pl.ds(pl.multiple_of(ss * own, 16), own)
            send(x_in.at[there], slab, slab_sem.at[0], slab_sem.at[1], to(i, t, ss)).start()
        slab[...] = x_in[pl.ds(pl.multiple_of(s * own, 16), own)]

    pl.semaphore_wait(far.at[0], z_near)
    signal_z(far.at[1])
    core_own.wait_recv()
    scaled = (xg[0].astype(f32) * half_gain[...]).astype(bf)
    xs[:, :per_device] = scaled
    xn[0] = scaled.T
    for k in range(CHUNKS):
        own_part[k] = jnp.dot(xn[0], w[k], preferred_element_type=f32)
    pl.semaphore_wait(far.at[1], z_near)
    signal_z(far.at[2])
    received(squares.at[pl.ds(1, 3)], sq_sem.at[1])
    total = squares[0] + squares[1] + squares[2] + squares[3]
    inv_row = lax.rsqrt(total[:1] / full + epsilon)
    inv_all = jnp.broadcast_to(inv_row, (per_device, per_device)).T[:, :1]
    back_load.wait()

    def send_d(r, k):
        start, size = LATE_GROUPS[r]
        these = pl.ds(start, size)
        copy = send(d_all.at[0, k, these], d_all.at[1, k, these], d_ssem, d_rsem.at[r, k], xdev)
        copy.start()
        d_sends[r, k] = copy

    row_cols = []
    for g, (start, size) in enumerate(SENT_GROUPS):
        here = slice(start, start + size)
        inv = inv_all[here]
        row_col = jnp.zeros((size, 1), f32)
        for k in range(CHUNKS):
            part_sends[g, k].wait_recv()
            raw_sums = own_part[k, here] + part_recv[k, here].astype(f32)
            gate, up = raw_sums[:, :ck] * inv, raw_sums[:, ck:] * inv
            grad = back[here, k * ck : (k + 1) * ck].astype(f32) * inv
            square = gate * gate
            tanh = jnp.tanh(SQRT_2_OVER_PI * gate * (1.0 + CUBIC * square))
            cdf = 0.5 * (1.0 + tanh)
            slope = cdf + 0.5 * gate * (1.0 - tanh * tanh) * (SQRT_2_OVER_PI * (1.0 + 3.0 * CUBIC * square))
            d_gate, d_up = grad * up * slope, grad * gate * cdf
            d_all[0, k, here, pl.ds(0, ck)] = d_gate.astype(bf)
            d_all[0, k, here, pl.ds(ck, ck)] = d_up.astype(bf)
            if g > 0:
                send_d(g - 1, k)
            terms = d_gate * raw_sums[:, :ck] + d_up * raw_sums[:, ck:]
            row_col = row_col + jnp.sum(terms, axis=1, keepdims=True)
        row_cols.append(row_col)
    for k in range(CHUNKS):
        send_d(n_late - 1, k)

    row_col = jnp.concatenate(row_cols, axis=0)
    rows[0] = jnp.broadcast_to(row_col, (per_device, per_device)).T[:8]
    pl.semaphore_wait(far.at[2], z_near)
    for dt in range(4):
        for ds in range(4):
            if dt + ds > 0:
                target = to(i, lax.rem(t + dt, 4), lax.rem(s + ds, 4))
                send(rows.at[0], rows.at[dt * 4 + ds], row_sem.at[0], row_sem.at[1], target).start()

    def scatter(parts, landing, n):
        for e in (1, 0):
            tt = 2 * i + lax.rem(t + e, 2)
            dt = lax.rem(tt - t + 4, 4)
            for dy in (1, 0):
                ss = across if dy else s
                r = lax.rem(tt, 2) * 2 + ss // 2
                slot = dt * 2 + dy
                copy = send(parts.at[r], landing.at[slot], piece_ssem.at[n], piece_rsem.at[n], to(i, tt, ss))
                if e == 0 and dy == 0:

                    @pl.when(reducer)
                    def _(r=r):
                        landing[0] = parts[r]

                    @pl.when(not_reducer)
                    def _(copy=copy):
                        copy.start()

                else:
                    copy.start()

    def scattered(parts, n):
        @pl.when(reducer)
        def _():
            sent(parts.at[pl.ds(0, 3)], piece_ssem.at[n])

        @pl.when(not_reducer)
        def _():
            sent(parts, piece_ssem.at[n])

    def gathered(landing, n):
        received(landing.at[pl.ds(1, 7)], piece_rsem.at[n])
        result = landing[0].astype(f32)
        for slot in range(1, 8):
            result = result + landing[slot].astype(f32)
        return result

    def d_normed(slot, start, size):
        total = None
        for k in range(CHUNKS):
            if slot == 1:
                d_sends[late_of[start], k].wait_recv()
            term = jnp.dot(d_all[slot, k, start : start + size], w_t[k], preferred_element_type=f32)
            total = term if total is None else total + term
            if slot == 1 and k == 0:
                finish(late_of[start] - 1)
        repeated = [total] * (per_device // size)
        return (jnp.concatenate(repeated, axis=0) if len(repeated) > 1 else total).T

    late_of = {start: r for r, (start, _) in enumerate(LATE_GROUPS)}
    turned = d_normed(0, 0, per_device)
    for r in range(8):
        own_pieces[r % 2, r // 2] = turned[r * own : (r + 1) * own].astype(bf)
    swaps = {-1: send(own_pieces.at[1 - q], own_sib, sib_ssem.at[n_late], sib_rsem.at[n_late], cdev)}
    swaps[-1].start()

    def finish(r):
        swaps[r].wait_recv()
        if r < 0:
            own_halved[...] = (own_pieces[q].astype(f32) + own_sib[...].astype(f32)).astype(bf)
            scatter(own_halved, own_incoming, n_late)
        else:
            pieces, sib_in, halved, incoming, _, _ = late_bufs[r]
            halved[...] = (pieces[q].astype(f32) + sib_in[...].astype(f32)).astype(bf)
            scatter(halved, incoming, r)

    def weight_grads(k):
        both = jnp.concatenate([d_all[0, k], d_all[1, k]], axis=0)
        cols = pl.ds(k * ck, ck)
        grads = jnp.dot(xs[...], both, preferred_element_type=f32).astype(bf)
        grad_gate[:, cols] = grads[:, :ck]
        grad_up[:, cols] = grads[:, ck:]

    def padded(value, height):
        short = height - value.shape[0]
        return jnp.concatenate([value, jnp.zeros((short, per_device), f32)], axis=0) if short else value

    for r, (start, size) in enumerate(LATE_GROUPS):
        turned = d_normed(1, start, size)
        pieces, sib_in = late_bufs[r][:2]
        cuts = spans(own, per_device // size)
        for p in range(8):
            parts = [padded(turned[p * own + at : p * own + at + n], cuts[0][1]) for at, n in cuts]
            pieces[p % 2, p // 2] = pick(parts, size).astype(bf)
        swaps[r] = send(pieces.at[1 - q], sib_in, sib_ssem.at[r], sib_rsem.at[r], cdev)
        swaps[r].start()
    weight_grads(0)
    finish(n_late - 1)
    for k in range(1, CHUNKS):
        weight_grads(k)
    received(rows.at[pl.ds(1, 15)], row_sem.at[1])
    row_sum = rows[0]
    for slot in range(1, 16):
        row_sum = row_sum + rows[slot]
    factor = inv_row * inv_row * row_sum[:1] / full

    @pl.when(s != t)
    def _():
        received(slab, slab_sem.at[1])

    mine = slab[...].astype(f32)
    gain_own = gain_col[pl.ds(pl.multiple_of((t * 4 + s) * own, 16), own)]

    def moves(r):
        return send(late_bufs[r][4], late_bufs[r][5], last_send.at[r], last_recv.at[r], xdev)

    gain_copy = send(gains.at[0], gains.at[1], last_send.at[n_late], last_recv.at[n_late], xdev)

    @pl.when(reducer)
    def _():
        d_own = gathered(own_incoming, n_late)
        grad_t[...] = (gain_own * d_own - mine * factor).astype(bf)
        prods[pl.ds(0, own)] = mine * d_own
        prods[pl.ds(own, prods.shape[0] - own)] = jnp.zeros((prods.shape[0] - own, per_device), f32)
        local = pl.multiple_of((lax.rem(t, 2) * 4 + s) * own, 16)
        theirs = xg[1, pl.ds(local, own)].astype(f32)
        for r, (start, size) in enumerate(LATE_GROUPS):
            d_late = gathered(late_bufs[r][3], r)
            late_bufs[r][4][...] = d_late.astype(bf)
            moves(r).start()
            cuts = spans(own, per_device // size)
            for j, (at, n) in enumerate(cuts):
                product = d_late[:n] * turn(theirs[at : at + n], j * size - start)
                inside = (lane >= j * size) & (lane < (j + 1) * size)
                prods[pl.ds(at, n)] += jnp.where(inside, product, 0.0)
        gains[0] = jnp.broadcast_to(jnp.sum(prods[...].T, axis=0, keepdims=True), gains.shape[1:])
        gain_copy.start()
        gain_out[...] = gains[0, :1, :own]

    def drain():
        @pl.when(half != i)
        def _():
            sent(x_in, tok_send.at[0])
            sent(x_in, tok_send.at[1])

        @pl.when(half == i)
        def _():
            sent(x_in, tok_send.at[0])

        sent(x_in, core_send.at[0])
        sent(x_in, core_send.at[1])

        @pl.when(s == t)
        def _():
            sent(x_in.at[pl.ds(0, 3 * own)], slab_sem.at[0])

        sent(squares.at[pl.ds(1, 3)], sq_sem.at[0])
        sent(part_send, part_ssem)
        sent(d_all.at[0], d_ssem)
        sent(rows.at[pl.ds(1, 15)], row_sem.at[0])
        for copy in swaps.values():
            copy.wait_send()
        scattered(own_halved, n_late)
        for r in range(n_late):
            scattered(late_bufs[r][2], r)

    drain()

    @pl.when(reducer)
    def _():
        for r in range(n_late):
            moves(r).wait_send()
        gain_copy.wait_send()

    @pl.when(not_reducer)
    def _():
        d_own = None
        for r, (start, size) in enumerate(LATE_GROUPS):
            moves(r).wait_recv()
            value = late_bufs[r][5][...].astype(f32)
            cuts = spans(own, per_device // size)
            turned = [turn(value[:n], start - j * size) for j, (at, n) in enumerate(cuts)]
            part = jnp.concatenate(turned, axis=0)
            d_own = part if d_own is None else jnp.where(lane >= start, part, d_own)
        grad_t[...] = (gain_own * d_own - mine * factor).astype(bf)
        gain_copy.wait_recv()
        gain_out[...] = gains[1, :1, :own]


WRITES = 4


def write_kernel(grad_t, gain, grad_gate, grad_up, grad_t_out, gain_out, gate_out, up_out, sems):
    pairs = [(grad_t, grad_t_out), (gain, gain_out)]
    n = grad_gate.shape[0] // WRITES
    for p in range(WRITES):
        part = pl.ds(p * n, n)
        pairs += [(grad_gate.at[part], gate_out.at[part]), (grad_up.at[part], up_out.at[part])]
    copies = [pltpu.make_async_copy(src, dst, sems.at[n]) for n, (src, dst) in enumerate(pairs)]
    for copy in copies:
        copy.start()
    for copy in copies:
        copy.wait()


def fused_shards(tokens, hidden_grad, norm_gain, w_gate, w_up):
    per_device, sec_rows = tokens.shape
    block, width = w_gate.shape
    full = norm_gain.shape[0]
    own = full // 16
    ck = width // CHUNKS
    bf, f32 = jnp.bfloat16, jnp.float32
    vmem = pl.BlockSpec(memory_space=pltpu.VMEM)
    anywhere = pl.BlockSpec(memory_space=pltpu.HBM)
    dma = pltpu.SemaphoreType.DMA
    own_pad = pl.cdiv(own, 128) * 128
    kept = (
        jax.ShapeDtypeStruct((own, per_device), bf),
        jax.ShapeDtypeStruct((1, own), f32),
        jax.ShapeDtypeStruct((block, width), bf),
        jax.ShapeDtypeStruct((block, width), bf),
    )
    n_sent, n_late = len(SENT_GROUPS), len(LATE_GROUPS)
    sent_rows = [sec_rows * size // per_device for _, size in SENT_GROUPS]
    late_rows = [spans(own, per_device // size)[0][1] for _, size in LATE_GROUPS]
    operands = (tokens.T, norm_gain.reshape(full // 128, 128), hidden_grad, w_gate, w_up)
    results = pl.pallas_call(
        functools.partial(exchange_kernel, full),
        out_shape=tuple(pltpu.VMEM(a.shape, a.dtype) for a in kept),
        in_specs=[anywhere] * 5,
        out_specs=(vmem,) * 4,
        scratch_shapes=[
            pltpu.VMEM((sec_rows, per_device), bf),
            [pltpu.VMEM((n, per_device), bf) for n in sent_rows],
            [pltpu.VMEM((2 * n, per_device), bf) for n in sent_rows],
            pltpu.VMEM((full // 128, 128), f32),
            pltpu.VMEM((full, 128), f32),
            pltpu.VMEM((CHUNKS, block, 2 * ck), bf),
            pltpu.VMEM((CHUNKS, 2 * ck, block), bf),
            pltpu.VMEM((per_device, width), bf),
            pltpu.VMEM((2, block, per_device), bf),
            pltpu.VMEM((block, 2 * per_device), bf),
            pltpu.VMEM((2, per_device, block), bf),
            pltpu.VMEM((own, per_device), bf),
            pltpu.VMEM((4, 8, per_device), f32),
            pltpu.VMEM((CHUNKS, per_device, 2 * ck), bf),
            pltpu.VMEM((CHUNKS, per_device, 2 * ck), bf),
            pltpu.VMEM((CHUNKS, per_device, 2 * ck), f32),
            pltpu.VMEM((2, CHUNKS, per_device, 2 * ck), bf),
            pltpu.VMEM((2, 4, own, per_device), bf),
            pltpu.VMEM((4, own, per_device), bf),
            pltpu.VMEM((4, own, per_device), bf),
            pltpu.VMEM((8, own, per_device), bf),
            [
                [pltpu.VMEM((*lead, n, per_device), bf) for lead in ((2, 4), (4,), (4,), (8,), (), ())]
                for n in late_rows
            ],
            pltpu.VMEM((16, 8, per_device), f32),
            pltpu.VMEM((own_pad, per_device), f32),
            pltpu.VMEM((2, 8, own_pad), f32),
            pltpu.SemaphoreType.REGULAR((3,)),
            dma((3,)),
            dma((2, CHUNKS)),
            dma((2,)),
            dma((n_sent + 1,)),
            dma((2,)),
            dma((n_sent + 1,)),
            dma((2,)),
            dma((2,)),
            dma,
            dma((n_sent, CHUNKS)),
            dma,
            dma((n_late, CHUNKS)),
            dma((n_late + 1,)),
            dma((n_late + 1,)),
            dma((n_late + 1,)),
            dma((n_late + 1,)),
            dma((n_late + 1,)),
            dma((n_late + 1,)),
            dma((2,)),
        ],
        compiler_params=pltpu.CompilerParams(
            collective_id=0, has_side_effects=True, vmem_limit_bytes=40 * 1024 * 1024
        ),
    )(*(pltpu.with_memory_space_constraint(a, pltpu.HBM) for a in operands))
    grad_t, gain, grad_gate, grad_up = pl.pallas_call(
        write_kernel,
        out_shape=kept,
        in_specs=[vmem] * 4,
        out_specs=(anywhere,) * 4,
        scratch_shapes=[dma((2 * WRITES + 2,))],
        compiler_params=pltpu.CompilerParams(vmem_limit_bytes=16 * 1024 * 1024),
    )(*results)
    return grad_t.T, gain.reshape(own), grad_gate, grad_up


def solution(mesh):
    in_specs = (
        P("dp", "section"),
        P("dp", ("tp", "section")),
        P(),
        P("dp", ("tp", "section")),
        P("dp", ("tp", "section")),
    )
    out_specs = (
        P("dp", ("tp", "section")),
        P(("tp", "section")),
        P("dp", ("tp", "section")),
        P("dp", ("tp", "section")),
    )
    sizes = tuple(mesh.shape[a] for a in ("dp", "tp", "section"))
    body = fused_shards if sizes == (2, 4, 4) else shards
    return jax.shard_map(body, mesh=mesh, in_specs=in_specs, out_specs=out_specs, check_vma=False)
```
